32 devices in a mesh: seq: 8 (over z, core), grp: 4 (over y, x).
Axes of the slice: x: 2, y: 2, z: 4, core: 2. Of those that a mesh axis runs over, the one named last changes fastest.
Arguments:
- tokens: bfloat16 [16384, 1536], P(('seq', 'grp')), may hold values from -6 to 6
- w_query: bfloat16 [1536, 768], replicated, may hold values from -0.15625 to 0.15625
- w_key: bfloat16 [1536, 768], replicated, may hold values from -0.15625 to 0.15625
- w_value: bfloat16 [1536, 768], replicated, may hold values from -0.15625 to 0.15625
- w_output: bfloat16 [768, 1536], replicated, may hold values from -0.21875 to 0.21875
- level_weights: float32 [9, 6], replicated, may hold values from 0.05 to 0.5
Outputs:
- mixed: bfloat16 [16384, 1536], P(('seq', 'grp'))
The draws below stay inside these ranges and needn't reach their ends.
All inputs are finite; a program needn't handle non-finite values.
Results may differ from the reference program's by a relative error of at most 0.013.
Values may be sent and summed in bfloat16 or wider, within the bound.
A program may use at most 128 MiB of HBM per device.

```python
import math
import jax
import jax.numpy as jnp
from jax import lax

D = 1536
HEADS = 6
HEAD_DIM = 128
LEVELS = 9
TOK_DEV = 512
INNER = 768
TOKENS = 16384
N_SEQ = 8
N_GRP = 4


def level_of(rng, shape, pieces, low, high):
    level = 1.0
    for position, shards_of in pieces:
        steps = jax.random.uniform(jax.random.fold_in(jax.random.fold_in(rng, 6), position), (shards_of,), jnp.float32, low / len(pieces), high / len(pieces))
        level = level * jnp.repeat(jnp.exp(steps), shape[position] // shards_of).reshape((-1,) + (1,) * (len(shape) - 1 - position))
    return level


def scatter_about(key, extent, deviation, limit, pieces=(), kind=jnp.bfloat16):
    entries = jax.random.normal(key, extent, jnp.float32) * deviation
    if len(pieces) > 0:
        entries = level_of(key, extent, pieces, -0.22, 0.18) * entries
    return jnp.clip(entries, min=-limit, max=limit).astype(kind)


def setup_inputs(seed: int = 0) -> dict:
    key_list = jax.random.split(jax.random.key(seed), 7)
    tokens = scatter_about(key_list[0], (TOKENS, D), 1.0, 6.0, ((0, 32),))
    w_query = scatter_about(key_list[1], (D, INNER), D ** -0.5, 0.15625)
    w_key = scatter_about(key_list[2], (D, INNER), D ** -0.5, 0.15625)
    w_value = scatter_about(key_list[3], (D, INNER), D ** -0.5, 0.15625)
    w_output = scatter_about(key_list[4], (INNER, D), INNER ** -0.5, 0.21875)
    level_weights = jnp.clip(jnp.exp(jax.random.uniform(key_list[5], (LEVELS, HEADS), jnp.float32, math.log(0.05), math.log(0.5))), 0.05, 0.5)
    return {"tokens": tokens, "w_query": w_query, "w_key": w_key, "w_value": w_value, "w_output": w_output, "level_weights": level_weights}


def unit_heads(matrix):
    return (matrix * lax.rsqrt(lax.optimization_barrier(jnp.sum(matrix * matrix, -1, keepdims=True)) + 1e-06)).astype(jnp.bfloat16)

def reference(tokens, w_query, w_key, w_value, w_output, level_weights):
    blocks = N_SEQ * N_GRP
    query = unit_heads(jnp.dot(tokens, w_query, preferred_element_type=jnp.float32).reshape(TOKENS, HEADS, HEAD_DIM))
    keys = unit_heads(jnp.dot(tokens, w_key, preferred_element_type=jnp.float32).reshape(TOKENS, HEADS, HEAD_DIM))
    values = jnp.dot(tokens, w_value, preferred_element_type=jnp.float32).astype(jnp.bfloat16).reshape(TOKENS, HEADS, HEAD_DIM)
    query_blocks = query.reshape(blocks, TOK_DEV, HEADS, HEAD_DIM)
    key_blocks = keys.reshape(blocks, TOK_DEV, HEADS, HEAD_DIM)
    value_blocks = values.reshape(blocks, TOK_DEV, HEADS, HEAD_DIM)
    states = jnp.einsum('prhd,prhe->phde', key_blocks.astype(jnp.float32), value_blocks.astype(jnp.float32))
    positions = jnp.arange(blocks, dtype=jnp.int32)
    combined = jnp.zeros((blocks, HEADS, HEAD_DIM, HEAD_DIM), jnp.float32)
    for level in range(blocks.bit_length() - 1):
        grouped = states.reshape(blocks >> level, 1 << level, HEADS, HEAD_DIM, HEAD_DIM).sum(1)
        sibling = jnp.maximum((positions >> level) - 1, 0).astype(jnp.int32)
        present = (positions >> level & 1).astype(jnp.float32)
        factor = level_weights[level + 1] * 2.0 ** (-0.5 * level)
        combined = combined + present[:, None, None, None] * factor[None, :, None, None] * grouped[sibling]
    combined = combined.astype(jnp.bfloat16)
    causal = jnp.arange(TOK_DEV)[:, None] >= jnp.arange(TOK_DEV)[None, :]

    def one_block(operands):
        block_query, block_keys, block_values, block_state = operands
        query32 = block_query.astype(jnp.float32)
        scores = jnp.einsum('thd,shd->hts', query32, block_keys.astype(jnp.float32))
        weights = (jnp.where(causal[None], scores, 0.0) * level_weights[0][:, None, None]).astype(jnp.bfloat16)
        inside = jnp.einsum('hts,she->the', weights.astype(jnp.float32), block_values.astype(jnp.float32))
        earlier = jnp.einsum('thd,hde->the', query32, block_state.astype(jnp.float32))
        return (inside + earlier).astype(jnp.bfloat16)
    attended = lax.map(one_block, (query_blocks, key_blocks, value_blocks, combined))
    attended = attended.reshape(TOKENS, INNER)
    return jnp.dot(attended, w_output, preferred_element_type=jnp.float32).astype(jnp.bfloat16)
```

```python
import functools

import jax
import jax.numpy as jnp
from jax import lax
from jax.experimental import pallas as pl
from jax.experimental.pallas import tpu as pltpu
from jax.sharding import PartitionSpec as P

F32 = jnp.float32
BF16 = jnp.bfloat16
MESH = pl.DeviceIdType.MESH
PAIR = 2


def dot(a, b, dims=((1,), (0,))):
    return lax.dot_general(a, b, (dims, ((), ())), preferred_element_type=F32)


def layer(
    members,
    planes,
    heads,
    tok_hbm,
    wq_hbm,
    wk_hbm,
    wv_hbm,
    wo_hbm,
    lw,
    out_hbm,
    tok,
    wq,
    wk,
    wv,
    wo,
    query,
    keys,
    values,
    inside,
    lower,
    shards,
    gathered,
    total,
    arrived,
    local,
    above,
    mine,
    combined,
    result,
    load_sem,
    out_sem,
    a_send,
    a_recv,
    b_send,
    b_recv,
    c_send,
    c_recv,
):
    rows = tok.shape[0]
    width = keys.shape[1] // heads
    chunks = heads // PAIR
    span = PAIR * width
    plane = 2 * members
    shard = shards.shape[2]
    plane_bits = plane.bit_length() - 1
    z_bits = planes.bit_length() - 1
    half = rows // 2

    seq = lax.axis_index("seq")
    grp = lax.axis_index("grp")
    z = lax.div(seq, 2)
    q = lax.rem(seq, 2) * members + grp

    def in_plane(index):
        return (z * 2 + lax.div(index, members), lax.rem(index, members))

    def up(distance):
        return (seq + 2 * distance, grp)

    barrier = pltpu.get_barrier_semaphore()
    for d in range(1, plane):
        pl.semaphore_signal(
            barrier, inc=1, device_id=in_plane(lax.rem(q + d, plane)), device_id_type=MESH
        )
    for d in range(1, planes):
        pl.semaphore_signal(
            barrier,
            inc=1,
            device_id=(lax.rem(z + d, planes) * 2 + lax.rem(seq, 2), grp),
            device_id_type=MESH,
        )

    loads = {}

    def load(name, source, target):
        loads[name] = pltpu.make_async_copy(source, target, load_sem.at[len(loads)])
        loads[name].start()

    def load_chunk(name, source, target, c):
        load((name, c), source.at[:, pl.ds(c * span, span)], target.at[c])

    load("tok0", tok_hbm.at[pl.ds(0, half)], tok.at[pl.ds(0, half)])
    load_chunk("k", wk_hbm, wk, 0)
    load("tok1", tok_hbm.at[pl.ds(half, half)], tok.at[pl.ds(half, half)])
    load_chunk("v", wv_hbm, wv, 0)
    for c in range(1, chunks):
        load_chunk("k", wk_hbm, wk, c)
        load_chunk("v", wv_hbm, wv, c)
    for c in range(chunks):
        load_chunk("q", wq_hbm, wq, c)
    load("o", wo_hbm, wo)

    def unit(block):
        parts = []
        for i in range(PAIR):
            head = block[:, i * width : (i + 1) * width]
            norm = lax.rsqrt(jnp.sum(head * head, -1, keepdims=True) + 1e-06)
            parts.append((head * norm).astype(BF16))
        return jnp.concatenate(parts, 1)

    def cols(c):
        return pl.ds(c * span, span)

    halves = [pl.ds(0, half), pl.ds(half, half)]

    def a_copy(c, slot, source, device):
        return pltpu.make_async_remote_copy(
            src_ref=shards.at[c, slot],
            dst_ref=gathered.at[c, source],
            send_sem=a_send.at[c, slot],
            recv_sem=a_recv.at[c, source],
            device_id=device,
            device_id_type=MESH,
        )

    def b_copy(c, d, device):
        return pltpu.make_async_remote_copy(
            src_ref=total.at[c],
            dst_ref=arrived.at[c, d],
            send_sem=b_send.at[c, d],
            recv_sem=b_recv.at[c, d],
            device_id=device,
            device_id_type=MESH,
        )

    def c_copy(c, slot, source, device):
        return pltpu.make_async_remote_copy(
            src_ref=mine.at[c, slot],
            dst_ref=combined.at[c, source],
            send_sem=c_send.at[c, slot],
            recv_sem=c_recv.at[c, source],
            device_id=device,
            device_id_type=MESH,
        )

    def states(c):
        parts = []
        for i, r in enumerate(halves):
            if c == 0:
                loads[f"tok{i}"].wait()
                if i == 0:
                    loads["k", c].wait()
            elif i == 0:
                loads["k", c].wait()
            keys[r, cols(c)] = unit(dot(tok[r, :], wk[c]))
        loads["v", c].wait()
        for i, r in enumerate(halves):
            v = dot(tok[r, :], wv[c]).astype(BF16)
            values[r, cols(c)] = v
            both = dot(keys[r, cols(c)], v, ((0,), (0,)))
            parts.append(
                [both[i * width : (i + 1) * width, i * width : (i + 1) * width] for i in range(PAIR)]
            )
        whole = []
        for i in range(PAIR):
            lower[c * PAIR + i] = parts[0][i]
            whole.append(parts[0][i] + parts[1][i])
        stacked = jnp.concatenate(whole, 0).reshape(plane, shard, width)
        shards[c] = stacked.astype(BF16)
        if c == 0:
            pl.semaphore_wait(barrier, plane - 1 + planes - 1)
        for d in range(1, plane):
            peer = lax.rem(q + d, plane)
            a_copy(c, peer, q, in_plane(peer)).start()
        gathered[c, q] = shards[c, q]

    def head_of(c):
        return c * PAIR + lax.div(q * shard, width)

    def factor(level, c):
        return lw[level + 1, head_of(c)] * (2.0 ** (-0.5 * level))

    def totals(c):
        for d in range(1, plane):
            peer = lax.rem(q + d, plane)
            a_copy(c, peer, peer, in_plane(peer)).wait_recv()
        sums = [gathered[c, i].astype(F32) for i in range(plane)]
        tree = [sums]
        while len(tree[-1]) > 1:
            last = tree[-1]
            tree.append([last[i] + last[i + 1] for i in range(0, len(last), 2)])
        total[c] = tree[-1][0].astype(BF16)
        for d in range(1, planes):

            @pl.when(z + d < planes)
            def _():
                b_copy(c, d, up(d)).start()

        factors = [factor(level, c) for level in range(plane_bits)]
        for i in range(plane):
            value = jnp.zeros((shard, width), F32)
            for level in range(plane_bits):
                if i >> level & 1:
                    value = value + factors[level] * tree[level][(i >> level) - 1]
            local[c, i] = value

    def combine(c):
        above[c] = jnp.zeros((shard, width), F32)
        for d in range(1, planes):

            @pl.when(z >= d)
            def _():
                level = jnp.int32(0)
                for bit in range(1, z_bits):
                    differ = lax.div(z, 2**bit) != lax.div(z - d, 2**bit)
                    level = level + jnp.where(differ, 1, 0)
                weight = jnp.float32(0.0)
                for bit in range(z_bits):
                    weight = jnp.where(level == bit, factor(plane_bits + bit, c), weight)
                b_copy(c, d, up(d)).wait_recv()
                above[c] = above[c] + weight * arrived[c, d].astype(F32)

        top = above[c]
        for i in range(plane):
            mine[c, i] = (local[c, i] + top).astype(BF16)
        for d in range(1, plane):
            peer = lax.rem(q + d, plane)
            c_copy(c, peer, q, in_plane(peer)).start()
        combined[c, q] = mine[c, q]

    def queries(c):
        loads["q", c].wait()
        for r in halves:
            query[r, cols(c)] = unit(dot(tok[r, :], wq[c]))

    causal = lax.broadcasted_iota(jnp.int32, (half, half), 0) >= lax.broadcasted_iota(
        jnp.int32, (half, half), 1
    )

    def attend(c):
        for i in range(PAIR):
            h = c * PAIR + i
            col = pl.ds(h * width, width)
            for r in halves:
                scores = dot(query[r, col], keys[r, col], ((1,), (1,)))
                weights = (jnp.where(causal, scores, 0.0) * lw[0, h]).astype(BF16)
                inside[r, col] = dot(weights, values[r, col])

    def finish(c):
        for d in range(1, plane):
            peer = lax.rem(q + d, plane)
            c_copy(c, peer, peer, in_plane(peer)).wait_recv()
        state = combined[c].astype(F32).reshape(span, width)
        for i in range(PAIR):
            h = c * PAIR + i
            col = pl.ds(h * width, width)
            first = state[i * width : (i + 1) * width]
            second = first + lw[0, h] * lower[h]
            for r, s in zip(halves, (first, second)):
                earlier = dot(query[r, col], s.astype(BF16))
                keys[r, col] = (inside[r, col] + earlier).astype(BF16)

    for c in range(chunks):
        states(c)
    for c in range(chunks):
        queries(c)
    for c in range(chunks):
        totals(c)
        attend(c)
    for c in range(chunks):
        combine(c)
    loads["o"].wait()
    for c in range(chunks):
        finish(c)
    outs = []
    for i, r in enumerate(halves):
        result[r, :] = dot(keys[r, :], wo[...]).astype(BF16)
        outs.append(pltpu.make_async_copy(result.at[r], out_hbm.at[r], out_sem.at[i]))
        outs[-1].start()

    for c in range(chunks):
        for d in range(1, plane):
            peer = lax.rem(q + d, plane)
            a_copy(c, peer, q, in_plane(peer)).wait_send()
            c_copy(c, peer, q, in_plane(peer)).wait_send()
        for d in range(1, planes):

            @pl.when(z + d < planes)
            def _():
                b_copy(c, d, up(d)).wait_send()

    for copy in outs:
        copy.wait()


def per_device(tokens, w_query, w_key, w_value, w_output, level_weights):
    rows, model = tokens.shape
    inner = w_query.shape[1]
    heads = level_weights.shape[1]
    width = inner // heads
    members = lax.axis_size("grp")
    planes = lax.axis_size("seq") // 2
    plane = 2 * members
    chunks = heads // PAIR
    span = PAIR * width
    shard = span // plane
    anywhere = pl.BlockSpec(memory_space=pl.ANY)
    vmem = pltpu.VMEM
    dma = pltpu.SemaphoreType.DMA
    return pl.pallas_call(
        functools.partial(layer, members, planes, heads),
        out_shape=jax.ShapeDtypeStruct((rows, w_output.shape[1]), BF16),
        in_specs=[anywhere] * 5 + [pl.BlockSpec(memory_space=pltpu.SMEM)],
        out_specs=anywhere,
        scratch_shapes=[
            vmem((rows, model), BF16),
            vmem((chunks, model, span), BF16),
            vmem((chunks, model, span), BF16),
            vmem((chunks, model, span), BF16),
            vmem((inner, w_output.shape[1]), BF16),
            vmem((rows, inner), BF16),
            vmem((rows, inner), BF16),
            vmem((rows, inner), BF16),
            vmem((rows, inner), F32),
            vmem((heads, width, width), F32),
            vmem((chunks, plane, shard, width), BF16),
            vmem((chunks, plane, shard, width), BF16),
            vmem((chunks, shard, width), BF16),
            vmem((chunks, planes, shard, width), BF16),
            vmem((chunks, plane, shard, width), F32),
            vmem((chunks, shard, width), F32),
            vmem((chunks, plane, shard, width), BF16),
            vmem((chunks, plane, shard, width), BF16),
            vmem((rows, w_output.shape[1]), BF16),
            dma((3 + 3 * chunks,)),
            dma((2,)),
            dma((chunks, plane)),
            dma((chunks, plane)),
            dma((chunks, planes)),
            dma((chunks, planes)),
            dma((chunks, plane)),
            dma((chunks, plane)),
        ],
        compiler_params=pltpu.CompilerParams(
            collective_id=0, has_side_effects=True, vmem_limit_bytes=62 * 2**20
        ),
    )(tokens, w_query, w_key, w_value, w_output, level_weights)


def solution(mesh):
    placed = (P(("seq", "grp"), None), P(), P(), P(), P(), P())
    return jax.shard_map(
        per_device, mesh=mesh, in_specs=placed, out_specs=P(("seq", "grp"), None), check_vma=False
    )
```

```python
import functools

import jax
import jax.numpy as jnp
from jax import lax
from jax.experimental import pallas as pl
from jax.experimental.pallas import tpu as pltpu
from jax.sharding import PartitionSpec as P

F32 = jnp.float32
BF16 = jnp.bfloat16
MESH = pl.DeviceIdType.MESH
PAIR = 2


def dot(a, b, dims=((1,), (0,))):
    return lax.dot_general(a, b, (dims, ((), ())), preferred_element_type=F32)


def layer(
    members,
    planes,
    heads,
    tok_hbm,
    wq_hbm,
    wk_hbm,
    wv_hbm,
    lw,
    out_hbm,
    tok,
    wq,
    wk,
    wv,
    query,
    keys,
    values,
    inside,
    lower,
    shards,
    gathered,
    total,
    arrived,
    local,
    above,
    mine,
    combined,
    load_sem,
    out_sem,
    a_send,
    a_recv,
    b_send,
    b_recv,
    c_send,
    c_recv,
):
    rows = tok.shape[0]
    width = keys.shape[1] // heads
    chunks = heads // PAIR
    span = PAIR * width
    plane = 2 * members
    shard = shards.shape[2]
    plane_bits = plane.bit_length() - 1
    z_bits = planes.bit_length() - 1
    half = rows // 2

    seq = lax.axis_index("seq")
    grp = lax.axis_index("grp")
    z = lax.div(seq, 2)
    q = lax.rem(seq, 2) * members + grp

    def in_plane(index):
        return (z * 2 + lax.div(index, members), lax.rem(index, members))

    def up(distance):
        return (seq + 2 * distance, grp)

    barrier = pltpu.get_barrier_semaphore()
    for d in range(1, plane):
        pl.semaphore_signal(
            barrier, inc=1, device_id=in_plane(lax.rem(q + d, plane)), device_id_type=MESH
        )
    for d in range(1, planes):
        pl.semaphore_signal(
            barrier,
            inc=1,
            device_id=(lax.rem(z + d, planes) * 2 + lax.rem(seq, 2), grp),
            device_id_type=MESH,
        )

    loads = {}

    def load(name, source, target):
        loads[name] = pltpu.make_async_copy(source, target, load_sem.at[len(loads)])
        loads[name].start()

    def load_chunk(name, source, target, c):
        load((name, c), source.at[:, pl.ds(c * span, span)], target.at[c])

    load("tok0", tok_hbm.at[pl.ds(0, half)], tok.at[pl.ds(0, half)])
    load_chunk("k", wk_hbm, wk, 0)
    load("tok1", tok_hbm.at[pl.ds(half, half)], tok.at[pl.ds(half, half)])
    load_chunk("v", wv_hbm, wv, 0)
    for c in range(1, chunks):
        load_chunk("k", wk_hbm, wk, c)
        load_chunk("v", wv_hbm, wv, c)
    for c in range(chunks):
        load_chunk("q", wq_hbm, wq, c)

    def unit(block):
        parts = []
        for i in range(PAIR):
            head = block[:, i * width : (i + 1) * width]
            norm = lax.rsqrt(jnp.sum(head * head, -1, keepdims=True) + 1e-06)
            parts.append((head * norm).astype(BF16))
        return jnp.concatenate(parts, 1)

    def cols(c):
        return pl.ds(c * span, span)

    halves = [pl.ds(0, half), pl.ds(half, half)]

    def a_copy(c, slot, source, device):
        return pltpu.make_async_remote_copy(
            src_ref=shards.at[c, slot],
            dst_ref=gathered.at[c, source],
            send_sem=a_send.at[c, slot],
            recv_sem=a_recv.at[c, source],
            device_id=device,
            device_id_type=MESH,
        )

    def b_copy(c, d, device):
        return pltpu.make_async_remote_copy(
            src_ref=total.at[c],
            dst_ref=arrived.at[c, d],
            send_sem=b_send.at[c, d],
            recv_sem=b_recv.at[c, d],
            device_id=device,
            device_id_type=MESH,
        )

    def c_copy(c, slot, source, device):
        return pltpu.make_async_remote_copy(
            src_ref=mine.at[c, slot],
            dst_ref=combined.at[c, source],
            send_sem=c_send.at[c, slot],
            recv_sem=c_recv.at[c, source],
            device_id=device,
            device_id_type=MESH,
        )

    def states(c):
        parts = []
        for i, r in enumerate(halves):
            if c == 0:
                loads[f"tok{i}"].wait()
                if i == 0:
                    loads["k", c].wait()
            elif i == 0:
                loads["k", c].wait()
            keys[r, cols(c)] = unit(dot(tok[r, :], wk[c]))
        loads["v", c].wait()
        for i, r in enumerate(halves):
            v = dot(tok[r, :], wv[c]).astype(BF16)
            values[r, cols(c)] = v
            both = dot(keys[r, cols(c)], v, ((0,), (0,)))
            parts.append(
                [both[i * width : (i + 1) * width, i * width : (i + 1) * width] for i in range(PAIR)]
            )
        whole = []
        for i in range(PAIR):
            lower[c * PAIR + i] = parts[0][i]
            whole.append(parts[0][i] + parts[1][i])
        stacked = jnp.concatenate(whole, 0).reshape(plane, shard, width)
        shards[c] = stacked.astype(BF16)
        if c == 0:
            pl.semaphore_wait(barrier, plane - 1 + planes - 1)
        for d in range(1, plane):
            peer = lax.rem(q + d, plane)
            a_copy(c, peer, q, in_plane(peer)).start()
        gathered[c, q] = shards[c, q]

    def head_of(c):
        return c * PAIR + lax.div(q * shard, width)

    def factor(level, c):
        return lw[head_of(c), level + 1] * (2.0 ** (-0.5 * level))

    def totals(c):
        for d in range(1, plane):
            peer = lax.rem(q + d, plane)
            a_copy(c, peer, peer, in_plane(peer)).wait_recv()
        sums = [gathered[c, i].astype(F32) for i in range(plane)]
        tree = [sums]
        while len(tree[-1]) > 1:
            last = tree[-1]
            tree.append([last[i] + last[i + 1] for i in range(0, len(last), 2)])
        total[c] = tree[-1][0].astype(BF16)
        for d in range(1, planes):

            @pl.when(z + d < planes)
            def _():
                b_copy(c, d, up(d)).start()

        factors = [factor(level, c) for level in range(plane_bits)]
        for i in range(plane):
            value = jnp.zeros((shard, width), F32)
            for level in range(plane_bits):
                if i >> level & 1:
                    value = value + factors[level] * tree[level][(i >> level) - 1]
            local[c, i] = value

    def combine(c):
        above[c] = jnp.zeros((shard, width), F32)
        for d in range(1, planes):

            @pl.when(z >= d)
            def _():
                level = jnp.int32(0)
                for bit in range(1, z_bits):
                    differ = lax.div(z, 2**bit) != lax.div(z - d, 2**bit)
                    level = level + jnp.where(differ, 1, 0)
                weight = jnp.float32(0.0)
                for bit in range(z_bits):
                    weight = jnp.where(level == bit, factor(plane_bits + bit, c), weight)
                b_copy(c, d, up(d)).wait_recv()
                above[c] = above[c] + weight * arrived[c, d].astype(F32)

        top = above[c]
        for i in range(plane):
            mine[c, i] = (local[c, i] + top).astype(BF16)
        for d in range(1, plane):
            peer = lax.rem(q + d, plane)
            c_copy(c, peer, q, in_plane(peer)).start()
        combined[c, q] = mine[c, q]

    def queries(c):
        loads["q", c].wait()
        for r in halves:
            query[r, cols(c)] = unit(dot(tok[r, :], wq[c]))

    causal = lax.broadcasted_iota(jnp.int32, (half, half), 0) >= lax.broadcasted_iota(
        jnp.int32, (half, half), 1
    )

    def attend(c):
        for i in range(PAIR):
            h = c * PAIR + i
            col = pl.ds(h * width, width)
            for r in halves:
                scores = dot(query[r, col], keys[r, col], ((1,), (1,)))
                weights = (jnp.where(causal, scores, 0.0) * lw[h, 0]).astype(BF16)
                inside[r, col] = dot(weights, values[r, col])

    def finish(c):
        for d in range(1, plane):
            peer = lax.rem(q + d, plane)
            c_copy(c, peer, peer, in_plane(peer)).wait_recv()
        state = combined[c].astype(F32).reshape(span, width)
        for i in range(PAIR):
            h = c * PAIR + i
            col = pl.ds(h * width, width)
            first = state[i * width : (i + 1) * width]
            second = first + lw[h, 0] * lower[h]
            for r, s in zip(halves, (first, second)):
                earlier = dot(query[r, col], s.astype(BF16))
                keys[r, col] = (inside[r, col] + earlier).astype(BF16)

    for c in range(chunks):
        states(c)
    for c in range(chunks):
        queries(c)
    for c in range(chunks):
        totals(c)
        attend(c)
    for c in range(chunks):
        combine(c)
    for c in range(chunks):
        finish(c)
    outs = []
    for i, r in enumerate(halves):
        outs.append(pltpu.make_async_copy(keys.at[r], out_hbm.at[r], out_sem.at[i]))
        outs[-1].start()

    for c in range(chunks):
        for d in range(1, plane):
            peer = lax.rem(q + d, plane)
            a_copy(c, peer, q, in_plane(peer)).wait_send()
            c_copy(c, peer, q, in_plane(peer)).wait_send()
        for d in range(1, planes):

            @pl.when(z + d < planes)
            def _():
                b_copy(c, d, up(d)).wait_send()

    for copy in outs:
        copy.wait()


def per_device(tokens, w_query, w_key, w_value, w_output, level_weights):
    rows, model = tokens.shape
    inner = w_query.shape[1]
    heads = level_weights.shape[1]
    width = inner // heads
    members = lax.axis_size("grp")
    planes = lax.axis_size("seq") // 2
    plane = 2 * members
    chunks = heads // PAIR
    span = PAIR * width
    shard = span // plane
    anywhere = pl.BlockSpec(memory_space=pl.ANY)
    vmem = pltpu.VMEM
    dma = pltpu.SemaphoreType.DMA
    attended = pl.pallas_call(
        functools.partial(layer, members, planes, heads),
        out_shape=jax.ShapeDtypeStruct((rows, inner), BF16),
        in_specs=[anywhere] * 4 + [pl.BlockSpec(memory_space=pltpu.SMEM)],
        out_specs=anywhere,
        scratch_shapes=[
            vmem((rows, model), BF16),
            vmem((chunks, model, span), BF16),
            vmem((chunks, model, span), BF16),
            vmem((chunks, model, span), BF16),
            vmem((rows, inner), BF16),
            vmem((rows, inner), BF16),
            vmem((rows, inner), BF16),
            vmem((rows, inner), F32),
            vmem((heads, width, width), F32),
            vmem((chunks, plane, shard, width), BF16),
            vmem((chunks, plane, shard, width), BF16),
            vmem((chunks, shard, width), BF16),
            vmem((chunks, planes, shard, width), BF16),
            vmem((chunks, plane, shard, width), F32),
            vmem((chunks, shard, width), F32),
            vmem((chunks, plane, shard, width), BF16),
            vmem((chunks, plane, shard, width), BF16),
            dma((3 + 3 * chunks,)),
            dma((2,)),
            dma((chunks, plane)),
            dma((chunks, plane)),
            dma((chunks, planes)),
            dma((chunks, planes)),
            dma((chunks, plane)),
            dma((chunks, plane)),
        ],
        compiler_params=pltpu.CompilerParams(
            collective_id=0, has_side_effects=True, vmem_limit_bytes=60*2**20
        ),
    )(tokens, w_query, w_key, w_value, level_weights.T)
    return dot(attended, w_output).astype(BF16)


def solution(mesh):
    placed = (P(("seq", "grp"), None), P(), P(), P(), P(), P())
    return jax.shard_map(
        per_device, mesh=mesh, in_specs=placed, out_specs=P(("seq", "grp"), None), check_vma=False
    )
```
